32 devices in a mesh: scene: 2 (over y), pulse: 8 (over z, x), scat: 2 (over core).
Axes of the slice: x: 2, y: 2, z: 4, core: 2. Of those that a mesh axis runs over, the one named last changes fastest.
Arguments:
- positions: float32 [32768], P(('scene', 'scat')), parts along dimension 0, may hold values from -1000 to 1000
- amplitude: float32 [2, 32768], P(None, ('scene', 'scat')), parts along dimension 1, may hold values from -3 to 3
- range_cells: int32 [32768], P(('scene', 'scat')), parts along dimension 0, may hold values from 0 to 1007
- bounce: int32 [32768], P(('scene', 'scat')), parts along dimension 0, may hold values 0 or 1
- stolt_block: int32 [512, 32], P(('pulse', 'scat')), may hold values from 0 to 30
- kernel_choice: int32 [512, 32], P(('pulse', 'scat')), may hold values from 0 to 15
- kernel_bank: float32 [16, 256, 128], replicated, may hold values from -0.375 to 0.375
Outputs:
- image: float32 [2, 1024, 4096], P(None, 'scene', ('pulse', 'scat')), parts along dimension 1
The draws below stay inside these ranges and needn't reach their ends.
There are 2 independent parts, one for each index of `scene`. The reference program is written for one: setup_inputs(seed, part) draws one part's arguments, and reference() takes and returns one part's arrays. A program takes and returns all parts, laid end to end along the dimension named above; an argument that names none is the same for every part. Nothing has to cross between parts.
All inputs are finite; a program needn't handle non-finite values. No bound on the sum of `bounce` on one device may be relied on, other than what follows from the above.
Results may differ from the reference program's by a relative error of at most 0.0003.
Values sent between devices are 32-bit elements; how exact they have to be, the bound alone decides.
A program may use at most 64 MiB of HBM per device.

```python
import jax
import jax.numpy as jnp
from jax import lax

P_SIZE = 512
SPECTRAL_BIN_LEN = 4096
B = 1024
SHIFT = 16
STOLT = 128
KERNELS = 16
S = 16384
BLOCKS = 32


def draw_positions(key, part):
    spread = jax.random.uniform(jax.random.fold_in(key, 11), (S,), jnp.float32, -1000.0, 1000.0)
    return spread.astype(jnp.float32)


def touch_ends(values, own_key, low, top_value):
    longest = values.shape.index(max(values.shape))
    spots = []
    for shift in (0, 1):
        where = [jax.random.randint(jax.random.fold_in(own_key, axis), (), 0, length) for axis, length in enumerate(values.shape)]
        where[longest] = (where[longest] + shift) % values.shape[longest]
        spots.append(tuple(where))
    return values.at[spots[0]].set(low).at[spots[1]].set(top_value)


def level_of(key, extent, shards, low, high):
    def one(dim, shards_of):
        draws = jax.random.uniform(jax.random.fold_in(jax.random.fold_in(key, 6), dim), (shards_of,), jnp.float32, low / len(shards), high / len(shards))
        return jnp.repeat(jnp.exp(draws), extent[dim] // shards_of).reshape((-1,) + (1,) * (len(extent) - dim - 1))

    level = one(*shards[0])
    for cut in shards[1:]:
        level = level * one(*cut)
    return level


def bell_draw(key, dims, deviation, bound, split=(), kind=jnp.bfloat16):
    values = deviation * jax.random.normal(key, dims, jnp.float32)
    if split:
        values = values * level_of(key, dims, split, -0.22, 0.18)
    return jnp.clip(values, -bound, bound).astype(kind)


def setup_inputs(seed: int = 0, part: int = 0) -> dict:
    keys = jax.random.split(jax.random.key(seed), 8)
    own_keys = jax.random.split(jax.random.fold_in(keys[7], part), 8)
    return {
        "positions": draw_positions(jax.random.fold_in(jax.random.fold_in(keys[7], part), 71), part),
        "amplitude": bell_draw(own_keys[1], (2, S), 0.5, 3.0, ((1, 2),), jnp.float32),
        "range_cells": touch_ends(jax.random.randint(own_keys[2], (S,), 0, B - SHIFT), jax.random.fold_in(own_keys[2], 1), 0, (B - SHIFT) - 1).astype(jnp.int32),
        "bounce": touch_ends((jax.random.randint(own_keys[3], (S,), 0, 4) < 1).astype(jnp.int32), jax.random.fold_in(own_keys[3], 1), 0, 1),
        "stolt_block": touch_ends(jax.random.randint(keys[4], (P_SIZE, BLOCKS), 0, BLOCKS - 1), jax.random.fold_in(keys[4], 1), 0, (BLOCKS - 1) - 1).astype(jnp.int32),
        "kernel_choice": touch_ends(jax.random.randint(keys[5], (P_SIZE, BLOCKS), 0, KERNELS), jax.random.fold_in(keys[5], 1), 0, KERNELS - 1).astype(jnp.int32),
        "kernel_bank": bell_draw(keys[6], (KERNELS, 2 * STOLT, STOLT), (2 * STOLT) ** -0.5, 0.375, (), jnp.float32),
    }


wavelength = 0.03125
spacing = 2.0
near_range = 700000.0
cell_size = 1.0
center_radio_tone = 9600000000.0
pulse_slope_rate = 150000000.0
wave_propagation_velocity = 300000000.0
highest_frequency = lax.Precision.HIGHEST

def steering(positions, amplitude, target, bounce, pulse_ids):
    along_track = (pulse_ids.astype(jnp.float32) - P_SIZE // 2) * spacing
    slant_range = near_range + cell_size * target.astype(jnp.float32)
    offset = along_track[:, None] - positions[None, :]
    excess = offset * offset / (jnp.sqrt(slant_range * slant_range + offset * offset) + slant_range)
    phase_angle = -4.0 * jnp.pi / wavelength * excess
    bounce_sign = 1.0 - 2.0 * bounce.astype(jnp.float32)
    real_part = bounce_sign * amplitude[0]
    imag_part = bounce_sign * amplitude[1]
    cos_part = jnp.cos(phase_angle)
    sin_part = jnp.sin(phase_angle)
    return (real_part * cos_part - imag_part * sin_part, real_part * sin_part + imag_part * cos_part)

def binning(steer_re, guiding_phasor_quadrature, target):
    stacked = jnp.concatenate([steer_re, guiding_phasor_quadrature], axis=0).T
    return jax.ops.segment_sum(stacked, target, num_segments=B)

def reference_phase(row_ids, matrix_slot_numbers):
    centered = (row_ids + P_SIZE // 2) % P_SIZE - P_SIZE // 2
    along_k = 2.0 * jnp.pi / (P_SIZE * spacing) * centered.astype(jnp.float32)
    slant_spatial_radian_rate = 4.0 * jnp.pi / wave_propagation_velocity * (center_radio_tone + (matrix_slot_numbers.astype(jnp.float32) - SPECTRAL_BIN_LEN // 2) * (pulse_slope_rate / SPECTRAL_BIN_LEN))
    squared = along_k * along_k
    depth = near_range + cell_size * (B // 2)
    return -depth * squared[:, None] / (jnp.sqrt(slant_spatial_radian_rate[None, :] * slant_spatial_radian_rate[None, :] - squared[:, None]) + slant_spatial_radian_rate[None, :])

def reference(positions, amplitude, range_cells, bounce, stolt_block, kernel_choice, kernel_bank):
    target = range_cells + SHIFT * bounce
    group_size = 64
    groups = jnp.arange(P_SIZE, dtype=jnp.int32).reshape(P_SIZE // group_size, group_size)

    def one_group(pulse_ids):
        steer_re, guiding_phasor_quadrature = steering(positions, amplitude, target, bounce, pulse_ids)
        return binning(steer_re, guiding_phasor_quadrature, target)
    binned = lax.map(one_group, groups)
    binned_re = binned[:, :, :group_size].transpose(0, 2, 1).reshape(P_SIZE, B)
    binned_im = binned[:, :, group_size:].transpose(0, 2, 1).reshape(P_SIZE, B)
    signal = jnp.pad(binned_re + 1j * binned_im, ((0, 0), (0, SPECTRAL_BIN_LEN - B)))
    echo = jnp.fft.fft(signal, axis=1)
    spectrum = jnp.fft.fft(echo, axis=0)
    phase_angle = reference_phase(jnp.arange(P_SIZE, dtype=jnp.int32), jnp.arange(SPECTRAL_BIN_LEN, dtype=jnp.int32))
    focused = spectrum * (jnp.cos(phase_angle) + 1j * jnp.sin(phase_angle))

    def window_pairs(row_data):
        tiled = row_data.reshape(BLOCKS, STOLT)
        return jnp.concatenate([tiled[:-1], tiled[1:]], axis=1)

    def stolt_row(row_item):
        row_re, row_im, first_blocks, kinds = row_item
        windows = jnp.stack([window_pairs(row_re), window_pairs(row_im)])
        chosen = windows[:, first_blocks, :]
        kernels = kernel_bank[kinds]
        result = jnp.einsum('cbu,but->cbt', chosen, kernels, precision=highest_frequency)
        return result.reshape(2, SPECTRAL_BIN_LEN)
    stolted = lax.map(stolt_row, (jnp.real(focused), jnp.imag(focused), stolt_block, kernel_choice))
    complex_rows = stolted[:, 0] + 1j * stolted[:, 1]
    ranged = jnp.fft.ifft(complex_rows, axis=1)
    image = jnp.fft.ifft(ranged, axis=0)
    return jnp.stack([jnp.real(image), jnp.imag(image)]).astype(jnp.float32)
```

```python
import functools

import jax
import jax.numpy as jnp
import numpy as np
from jax import lax
from jax.experimental import pallas as pl
from jax.experimental.pallas import tpu as pltpu
from jax.sharding import PartitionSpec as P

P_SIZE = 512
F_LEN = 4096
B = 1024
SHIFT = 16
STOLT = 128
BLOCKS = 32
SPACING = 2.0
NEAR = 700000.0
BIN_SIDE = 32
GROUP = 4
HIGH = lax.Precision.HIGH
f32 = jnp.float32
bf16 = jnp.bfloat16


def trig_coefs():
    x = np.cos(np.pi * (np.arange(400) + 0.5) / 400) * 0.5
    u = x * x
    s = np.polynomial.chebyshev.Chebyshev.fit(u, np.sin(np.pi * x) / x, 5).convert(
        kind=np.polynomial.Polynomial
    )
    c = np.polynomial.chebyshev.Chebyshev.fit(u, np.cos(np.pi * x), 5).convert(
        kind=np.polynomial.Polynomial
    )
    return [float(v) for v in s.coef], [float(v) for v in c.coef]


def horner(u, coefs):
    acc = jnp.full_like(u, coefs[-1])
    for c in coefs[-2::-1]:
        acc = acc * u + c
    return acc


def split(x):
    hi = x.astype(bf16)
    lo = (x - hi.astype(f32)).astype(bf16)
    return hi, lo


def np_split(x):
    x = np.asarray(x, np.float64)
    hi = np.asarray(x, jnp.bfloat16)
    lo = np.asarray(x - hi.astype(np.float64), jnp.bfloat16)
    return np.stack([hi, lo])


def dots(a, b, dims):
    d = functools.partial(
        lax.dot_general, dimension_numbers=(dims, ((), ())), preferred_element_type=f32
    )
    return d(a[0], b[0]) + (d(a[0], b[1]) + d(a[1], b[0]))


def bin_kernel(pulse_base, pos, amp, tgt, bnc, out, acc, *, pulses, sin_c, cos_c):
    step = pl.program_id(0)
    width = pos.shape[1]

    @pl.when(step == 0)
    def _():
        acc[...] = jnp.zeros_like(acc)

    base = pulse_base[0]
    ids = base + lax.broadcasted_iota(jnp.int32, (pulses, width), 0)
    along = (ids.astype(f32) - P_SIZE // 2) * SPACING
    target = tgt[...]
    slant = NEAR + target.astype(f32)
    offset = along - pos[...]
    square = offset * offset
    excess = square / (jnp.sqrt(slant * slant + square) + slant)
    halves = excess * -128.0
    whole = jnp.round(halves)
    r = halves - whole
    u = r * r
    odd = whole - 2.0 * jnp.floor(whole * 0.5)
    sign = 1.0 - 2.0 * odd
    sin_p = sign * r * horner(u, sin_c)
    cos_p = sign * horner(u, cos_c)
    flip = 1.0 - 2.0 * bnc[...].astype(f32)
    are = flip * amp[0:1]
    aim = flip * amp[1:2]
    re = are * cos_p - aim * sin_p
    im = are * sin_p + aim * cos_p
    steer = jnp.concatenate([re, im], 0)
    hi, lo = split(steer)
    rhs = jnp.concatenate([hi, lo], 0)
    bins = lax.broadcasted_iota(jnp.int32, (B, width), 0)
    hot = jnp.where(bins == target, 1.0, 0.0).astype(bf16)
    acc[...] += lax.dot_general(
        hot, rhs, (((1,), (1,)), ((), ())), preferred_element_type=f32
    )

    @pl.when(step == pl.num_programs(0) - 1)
    def _():
        out[...] = acc[:, : 2 * pulses] + acc[:, 2 * pulses :]


def binning(positions, amplitude, target, bounce, pulse_base, pulses):
    count = positions.shape[0]
    width = min(512, count)
    sin_c, cos_c = trig_coefs()
    row = lambda n: pl.BlockSpec((n, width), lambda i: (0, i))
    return pl.pallas_call(
        functools.partial(bin_kernel, pulses=pulses, sin_c=sin_c, cos_c=cos_c),
        grid=(count // width,),
        in_specs=[pl.BlockSpec(memory_space=pltpu.SMEM), row(1), row(2), row(1), row(1)],
        out_specs=pl.BlockSpec((B, 2 * pulses), lambda i: (0, 0)),
        out_shape=jax.ShapeDtypeStruct((B, 2 * pulses), f32),
        scratch_shapes=[pltpu.VMEM((B, 4 * pulses), f32)],
        name="binning",
    )(
        pulse_base.reshape(1),
        positions.reshape(1, count),
        amplitude,
        target.reshape(1, count),
        bounce.reshape(1, count),
    )


def complex_rows(c, s):
    return np.block([[c, s], [-s, c]])


def mid_tables(n_dev):
    side = np.arange(BIN_SIDE)
    t = np.arange(STOLT)
    eye = np.eye(GROUP)
    a = -2 * np.pi / STOLT * ((side[:, None] * t[None, :]) % STOLT)
    ta = complex_rows(np.cos(a), np.sin(a))
    a = -2 * np.pi / F_LEN * (side[:, None] * t[None, :])
    wa = np.stack([np.tile(np.cos(a), (GROUP, 1)), np.tile(np.sin(a), (GROUP, 1))])
    a = -2 * np.pi / BIN_SIDE * ((side[:, None] * side[None, :]) % BIN_SIDE)
    c, s = np.kron(eye, np.cos(a)), np.kron(eye, np.sin(a))
    tb = complex_rows(c, s).T
    blk = np.arange(BLOCKS)
    a = 2 * np.pi / BLOCKS * ((blk[:, None] * blk[None, :]) % BLOCKS)
    c, s = np.kron(eye, np.cos(a)), np.kron(eye, np.sin(a))
    tc = complex_rows(c, s)
    a = 2 * np.pi / F_LEN * (t[:, None] * blk[None, :])
    wc = np.stack([np.tile(np.cos(a), (1, GROUP)), np.tile(np.sin(a), (1, GROUP))])
    a = 2 * np.pi / STOLT * ((t[:, None] * t[None, :]) % STOLT)
    td = complex_rows(np.cos(a), np.sin(a)).T / F_LEN
    td = td.reshape(2, n_dev, STOLT // n_dev, 2 * STOLT).transpose(1, 0, 2, 3)
    td = td.reshape(2 * STOLT, 2 * STOLT)
    return (
        np_split(ta),
        wa.astype(np.float32),
        np_split(tb),
        np_split(tc),
        wc.astype(np.float32),
        np_split(td),
    )


def mid_kernel(x, phase, hot, kind, bank, ta, wa, tb, tc, wc, td, out, *, subs):
    n = GROUP * BLOCKS
    parts_hi, parts_lo = [], []
    for g in range(subs):
        lanes = slice(g * n, (g + 1) * n)
        y = dots(split(x[:, lanes]), (ta[0], ta[1]), ((0,), (0,)))
        yr, yi = y[:, :STOLT], y[:, STOLT:]
        y = jnp.concatenate([yr * wa[0] - yi * wa[1], yr * wa[1] + yi * wa[0]], 0)
        z = dots((tb[0], tb[1]), split(y), ((1,), (0,)))
        zr, zi = z[:n], z[n:]
        cp, sp = phase[0, lanes], phase[1, lanes]
        z = jnp.concatenate([zr * cp - zi * sp, zr * sp + zi * cp], 1)
        hi, lo = split(z)
        picked = jnp.dot(
            hot[g], jnp.concatenate([hi, lo], 1), preferred_element_type=f32
        ).astype(bf16)
        first, second = picked[:n], picked[n:]
        for c in range(2):
            for base, keep in ((0, parts_hi), (2 * STOLT, parts_lo)):
                cut = slice(base + c * STOLT, base + (c + 1) * STOLT)
                keep.append(jnp.concatenate([first[:, cut], second[:, cut]], 1))
    ghi = jnp.concatenate(parts_hi, 0)
    glo = jnp.concatenate(parts_lo, 0)
    kinds = kind[...].reshape(subs * 2 * n, 1)
    kinds = jnp.broadcast_to(kinds, (subs * 2 * n, STOLT))
    acc = jnp.zeros((subs * 2 * n, STOLT), f32)
    for k in range(bank.shape[1]):
        r = dots((ghi, glo), (bank[0, k], bank[1, k]), ((1,), (0,)))
        for half in range(2):
            acc = jnp.where(kinds == 2 * k + half, r[:, half * STOLT : (half + 1) * STOLT], acc)
    for g in range(subs):
        s = acc[g * 2 * n : (g + 1) * 2 * n]
        y = dots(split(s), (tc[0], tc[1]), ((0,), (0,)))
        yr, yi = y[:, :n], y[:, n:]
        y = jnp.concatenate([yr * wc[0] - yi * wc[1], yr * wc[1] + yi * wc[0]], 0)
        out[:, g * n : (g + 1) * n] = dots((td[0], td[1]), split(y), ((1,), (0,)))


def middle(x, phase, hot, kind, bank, tables):
    rows = x.shape[1] // BIN_SIDE
    groups = rows // GROUP
    subs = min(2, groups)
    n = GROUP * BLOCKS
    whole = lambda a: pl.BlockSpec(a.shape, lambda i: (0,) * a.ndim)
    return pl.pallas_call(
        functools.partial(mid_kernel, subs=subs),
        grid=(groups // subs,),
        in_specs=[
            pl.BlockSpec((x.shape[0], subs * n), lambda i: (0, i)),
            pl.BlockSpec((2, subs * n, STOLT), lambda i: (0, i, 0)),
            pl.BlockSpec((subs, 2 * n, n), lambda i: (i, 0, 0)),
            pl.BlockSpec((subs, 2 * n, 1), lambda i: (i, 0, 0)),
            whole(bank),
        ]
        + [whole(t) for t in tables],
        out_specs=pl.BlockSpec((2 * STOLT, subs * n), lambda i: (0, i)),
        out_shape=jax.ShapeDtypeStruct((2 * STOLT, groups * n), f32),
        name="middle",
    )(x, phase, hot, kind, bank, *tables)


def reference_phase(row_ids, cols):
    centered = (row_ids + P_SIZE // 2) % P_SIZE - P_SIZE // 2
    along_k = 2.0 * jnp.pi / (P_SIZE * SPACING) * centered.astype(f32)
    kr = 4.0 * jnp.pi / 3e8 * (9.6e9 + (cols.astype(f32) - F_LEN // 2) * (1.5e8 / F_LEN))
    squared = along_k * along_k
    depth = NEAR + B // 2
    return (
        -depth
        * squared[:, None]
        / (jnp.sqrt(kr[None, :] * kr[None, :] - squared[:, None]) + kr[None, :])
    )


def on_device(positions, amplitude, range_cells, bounce, stolt_block, kernel_choice, kernel_bank):
    n_pulse = lax.axis_size("pulse")
    n_scat = lax.axis_size("scat")
    n_dev = n_pulse * n_scat
    pulse_here = lax.axis_index("pulse")
    scat_here = lax.axis_index("scat")
    pulses = P_SIZE // n_pulse
    rows = P_SIZE // n_dev
    width = F_LEN // n_dev
    groups = rows // GROUP
    n = GROUP * BLOCKS
    bins_scat = B // n_scat
    bins_here = bins_scat // n_pulse

    ids = jnp.arange(GROUP, dtype=jnp.int32)[None, :, None] * BLOCKS
    first = stolt_block.reshape(groups, GROUP, BLOCKS) + ids
    pick = jnp.stack([first, first + 1], 1).reshape(groups, 2 * n, 1)
    hot = (pick == jnp.arange(n, dtype=jnp.int32)[None, None, :]).astype(bf16)
    kind = jnp.stack([kernel_choice.reshape(groups, n)] * 2, 1).reshape(groups, 2 * n, 1)
    kernels = kernel_bank.shape[0]
    bank = kernel_bank.reshape(kernels // 2, 2, 2 * STOLT, STOLT).transpose(0, 2, 1, 3)
    bank = bank.reshape(kernels // 2, 2 * STOLT, 2 * STOLT)
    bank_hi = lax.reduce_precision(bank, 8, 7)
    bank = jnp.stack([bank_hi.astype(bf16), (bank - bank_hi).astype(bf16)])
    row_ids = (pulse_here * n_scat + scat_here) * rows + jnp.arange(rows, dtype=jnp.int32)
    theta = reference_phase(row_ids, jnp.arange(F_LEN, dtype=jnp.int32))
    theta = theta.reshape(rows * BLOCKS, STOLT)
    phase = jnp.stack([jnp.cos(theta), jnp.sin(theta)])

    target = range_cells + SHIFT * bounce
    partial = binning(positions, amplitude, target, bounce, pulse_here * pulses, pulses)
    partial = partial.reshape(n_scat, bins_scat, 2 * pulses)
    binned = lax.dynamic_index_in_dim(partial, scat_here, 0, keepdims=False)
    for shift in range(1, n_scat):
        other = lax.dynamic_index_in_dim(
            partial, (scat_here + shift) % n_scat, 0, keepdims=False
        )
        ring = [(i, (i + shift) % n_scat) for i in range(n_scat)]
        binned = binned + lax.ppermute(other, "scat", ring)

    turned = lax.all_to_all(
        binned.reshape(n_pulse, bins_here, 2 * pulses), "pulse", 0, 0, tiled=True
    )
    turned = turned.reshape(n_pulse, bins_here, 2, pulses).transpose(0, 3, 2, 1)
    turned = turned.reshape(P_SIZE, 2 * bins_here)
    k = np.arange(P_SIZE)
    angle = 2 * np.pi / P_SIZE * ((k[:, None] * k[None, :]) % P_SIZE)
    az = jnp.asarray(np.concatenate([np.cos(angle), np.sin(angle)], 0), f32)
    product = jnp.dot(az, turned, precision=HIGH, preferred_element_type=f32)
    pc, ps = product[:P_SIZE], product[P_SIZE:]
    spectrum = pc + jnp.concatenate([ps[:, bins_here:], -ps[:, :bins_here]], 1)

    az_rows = lax.all_to_all(
        spectrum.reshape(n_dev, rows, 2 * bins_here), ("pulse", "scat"), 0, 0, tiled=True
    )
    x = az_rows.reshape(n_pulse, n_scat, rows, 2, bins_here).transpose(3, 1, 0, 4, 2)
    x = x.reshape(2, BIN_SIDE, BIN_SIDE, rows).transpose(0, 1, 3, 2)
    x = x.reshape(2 * BIN_SIDE, rows * BIN_SIDE)
    tables = tuple(jnp.asarray(t) for t in mid_tables(n_dev))
    ranged = middle(x, phase, hot, kind, bank, tables)

    per = STOLT // n_dev
    columns = lax.all_to_all(
        ranged.reshape(n_dev, 2 * per, rows * BLOCKS), ("pulse", "scat"), 0, 0, tiled=True
    )
    columns = columns.reshape(n_dev, 2, per, rows, BLOCKS).transpose(0, 3, 1, 2, 4)
    columns = columns.reshape(P_SIZE, 2 * width)
    final = jnp.dot(az, columns, precision=HIGH, preferred_element_type=f32)
    fc, fs = final[:P_SIZE], final[P_SIZE:]
    re = (fc[:, :width] - fs[:, width:]) / P_SIZE
    im = (fc[:, width:] + fs[:, :width]) / P_SIZE
    return jnp.stack([re, im])


def solution(mesh):
    placed = (
        P(("scene", "scat")),
        P(None, ("scene", "scat")),
        P(("scene", "scat")),
        P(("scene", "scat")),
        P(("pulse", "scat"), None),
        P(("pulse", "scat"), None),
        P(),
    )
    return jax.shard_map(
        on_device,
        mesh=mesh,
        in_specs=placed,
        out_specs=P(None, "scene", ("pulse", "scat")),
        check_vma=False,
    )
```

```python
import functools

import jax
import jax.numpy as jnp
import numpy as np
from jax import lax
from jax.experimental import pallas as pl
from jax.experimental.pallas import tpu as pltpu
from jax.sharding import PartitionSpec as P

P_SIZE = 512
F_LEN = 4096
B = 1024
SHIFT = 16
STOLT = 128
BLOCKS = 32
SPACING = 2.0
NEAR = 700000.0
BIN_SIDE = 32
GROUP = 4
HIGH = lax.Precision.HIGH
f32 = jnp.float32
bf16 = jnp.bfloat16


def trig_coefs():
    x = np.cos(np.pi * (np.arange(400) + 0.5) / 400) * 0.5
    u = x * x
    s = np.polynomial.chebyshev.Chebyshev.fit(u, np.sin(np.pi * x) / x, 5).convert(
        kind=np.polynomial.Polynomial
    )
    c = np.polynomial.chebyshev.Chebyshev.fit(u, np.cos(np.pi * x), 5).convert(
        kind=np.polynomial.Polynomial
    )
    return [float(v) for v in s.coef], [float(v) for v in c.coef]


def horner(u, coefs):
    acc = jnp.full_like(u, coefs[-1])
    for c in coefs[-2::-1]:
        acc = acc * u + c
    return acc


def split(x):
    hi = x.astype(bf16)
    lo = (x - hi.astype(f32)).astype(bf16)
    return hi, lo


def np_split(x):
    x = np.asarray(x, np.float64)
    hi = np.asarray(x, jnp.bfloat16)
    lo = np.asarray(x - hi.astype(np.float64), jnp.bfloat16)
    return np.stack([hi, lo])


def dots(a, b, dims):
    d = functools.partial(
        lax.dot_general, dimension_numbers=(dims, ((), ())), preferred_element_type=f32
    )
    return d(a[0], b[0]) + (d(a[0], b[1]) + d(a[1], b[0]))


def bin_kernel(pulse_base, pos, amp, tgt, bnc, out, acc, *, pulses, sin_c, cos_c):
    step = pl.program_id(0)
    width = pos.shape[1]

    @pl.when(step == 0)
    def _():
        acc[...] = jnp.zeros_like(acc)

    base = pulse_base[0]
    ids = base + lax.broadcasted_iota(jnp.int32, (pulses, width), 0)
    along = (ids.astype(f32) - P_SIZE // 2) * SPACING
    target = tgt[...]
    slant = NEAR + target.astype(f32)
    offset = along - pos[...]
    square = offset * offset
    excess = square / (jnp.sqrt(slant * slant + square) + slant)
    halves = excess * -128.0
    whole = jnp.round(halves)
    r = halves - whole
    u = r * r
    odd = whole - 2.0 * jnp.floor(whole * 0.5)
    sign = 1.0 - 2.0 * odd
    sin_p = sign * r * horner(u, sin_c)
    cos_p = sign * horner(u, cos_c)
    flip = 1.0 - 2.0 * bnc[...].astype(f32)
    are = flip * amp[0:1]
    aim = flip * amp[1:2]
    re = are * cos_p - aim * sin_p
    im = are * sin_p + aim * cos_p
    steer = jnp.concatenate([re, im], 0)
    hi, lo = split(steer)
    rhs = jnp.concatenate([hi, lo], 0)
    bins = lax.broadcasted_iota(jnp.int32, (B, width), 0)
    hot = jnp.where(bins == target, 1.0, 0.0).astype(bf16)
    acc[...] += lax.dot_general(
        hot, rhs, (((1,), (1,)), ((), ())), preferred_element_type=f32
    )

    @pl.when(step == pl.num_programs(0) - 1)
    def _():
        out[...] = acc[:, : 2 * pulses] + acc[:, 2 * pulses :]


def binning(positions, amplitude, target, bounce, pulse_base, pulses):
    count = positions.shape[0]
    width = min(512, count)
    sin_c, cos_c = trig_coefs()
    row = lambda n: pl.BlockSpec((n, width), lambda i: (0, i))
    return pl.pallas_call(
        functools.partial(bin_kernel, pulses=pulses, sin_c=sin_c, cos_c=cos_c),
        grid=(count // width,),
        in_specs=[pl.BlockSpec(memory_space=pltpu.SMEM), row(1), row(2), row(1), row(1)],
        out_specs=pl.BlockSpec((B, 2 * pulses), lambda i: (0, 0)),
        out_shape=jax.ShapeDtypeStruct((B, 2 * pulses), f32),
        scratch_shapes=[pltpu.VMEM((B, 4 * pulses), f32)],
        name="binning",
    )(
        pulse_base.reshape(1),
        positions.reshape(1, count),
        amplitude,
        target.reshape(1, count),
        bounce.reshape(1, count),
    )


def complex_rows(c, s):
    return np.block([[c, s], [-s, c]])


def mid_tables(n_dev, order):
    side = np.arange(BIN_SIDE)
    t = np.arange(STOLT)
    eye = np.eye(GROUP)
    a = -2 * np.pi / STOLT * ((side[:, None] * t[None, :]) % STOLT)
    ta = complex_rows(np.cos(a), np.sin(a))[order]
    a = -2 * np.pi / F_LEN * (side[:, None] * t[None, :])
    wa = np.stack([np.tile(np.cos(a), (GROUP, 1)), np.tile(np.sin(a), (GROUP, 1))])
    a = -2 * np.pi / BIN_SIDE * ((side[:, None] * side[None, :]) % BIN_SIDE)
    c, s = np.kron(eye, np.cos(a)), np.kron(eye, np.sin(a))
    tb = complex_rows(c, s).T
    blk = np.arange(BLOCKS)
    a = 2 * np.pi / BLOCKS * ((blk[:, None] * blk[None, :]) % BLOCKS)
    c, s = np.kron(eye, np.cos(a)), np.kron(eye, np.sin(a))
    tc = complex_rows(c, s)
    a = 2 * np.pi / F_LEN * (t[:, None] * blk[None, :])
    wc = np.stack([np.tile(np.cos(a), (1, GROUP)), np.tile(np.sin(a), (1, GROUP))])
    a = 2 * np.pi / STOLT * ((t[:, None] * t[None, :]) % STOLT)
    td = complex_rows(np.cos(a), np.sin(a)).T / F_LEN
    td = td.reshape(2, n_dev, STOLT // n_dev, 2 * STOLT).transpose(1, 0, 2, 3)
    td = td.reshape(2 * STOLT, 2 * STOLT)
    return (
        np_split(ta),
        wa.astype(np.float32),
        np_split(tb),
        np_split(tc),
        wc.astype(np.float32),
        np_split(td),
    )


def mid_kernel(
    x, cos_p, sin_p, hot, kind, bank_hi, bank_lo, ta, wa, tb, tc, wc, td, out, xs, os, *, subs
):
    n = GROUP * BLOCKS
    step = pl.program_id(0)
    groups = x.shape[1]

    @pl.when(step == 0)
    def _():
        for g in range(groups):
            xs[g] = x[:, g, :]

    parts_hi, parts_lo = [], []
    for g in range(subs):
        lanes = slice(g * n, (g + 1) * n)
        y = dots(split(xs[step * subs + g]), (ta[0], ta[1]), ((0,), (0,)))
        yr, yi = y[:, :STOLT], y[:, STOLT:]
        y = jnp.concatenate([yr * wa[0] - yi * wa[1], yr * wa[1] + yi * wa[0]], 0)
        z = dots((tb[0], tb[1]), split(y), ((1,), (0,)))
        zr, zi = z[:n], z[n:]
        cp, sp = cos_p[lanes], sin_p[lanes]
        z = jnp.concatenate([zr * cp - zi * sp, zr * sp + zi * cp], 1)
        hi, lo = split(z)
        picked = jnp.dot(
            hot[g], jnp.concatenate([hi, lo], 1), preferred_element_type=f32
        ).astype(bf16)
        first, second = picked[:n], picked[n:]
        for c in range(2):
            for base, keep in ((0, parts_hi), (2 * STOLT, parts_lo)):
                cut = slice(base + c * STOLT, base + (c + 1) * STOLT)
                keep.append(jnp.concatenate([first[:, cut], second[:, cut]], 1))
    ghi = jnp.concatenate(parts_hi, 0)
    glo = jnp.concatenate(parts_lo, 0)
    kinds = kind[...].reshape(subs * 2 * n, 1)
    kinds = jnp.broadcast_to(kinds, (subs * 2 * n, STOLT))
    acc = jnp.zeros((subs * 2 * n, STOLT), f32)
    for k in range(0, bank_hi.shape[0], 2):
        khi = jnp.concatenate([bank_hi[k], bank_hi[k + 1]], 1)
        klo = jnp.concatenate([bank_lo[k], bank_lo[k + 1]], 1)
        r = dots((ghi, glo), (khi, klo), ((1,), (0,)))
        for half in range(2):
            acc = jnp.where(kinds == k + half, r[:, half * STOLT : (half + 1) * STOLT], acc)
    for g in range(subs):
        s = acc[g * 2 * n : (g + 1) * 2 * n]
        y = dots(split(s), (tc[0], tc[1]), ((0,), (0,)))
        yr, yi = y[:, :n], y[:, n:]
        y = jnp.concatenate([yr * wc[0] - yi * wc[1], yr * wc[1] + yi * wc[0]], 0)
        os[step * subs + g] = dots((td[0], td[1]), split(y), ((1,), (0,)))

    @pl.when(step == pl.num_programs(0) - 1)
    def _():
        for g in range(groups):
            out[:, g, :] = os[g]


def middle(x, cos_p, sin_p, hot, kind, bank_hi, bank_lo, tables):
    groups = x.shape[1]
    subs = min(2, groups)
    n = GROUP * BLOCKS
    whole = lambda a: pl.BlockSpec(a.shape, lambda i: (0,) * a.ndim)
    return pl.pallas_call(
        functools.partial(mid_kernel, subs=subs),
        grid=(groups // subs,),
        in_specs=[
            whole(x),
            pl.BlockSpec((subs * n, STOLT), lambda i: (i, 0)),
            pl.BlockSpec((subs * n, STOLT), lambda i: (i, 0)),
            pl.BlockSpec((subs, 2 * n, n), lambda i: (i, 0, 0)),
            pl.BlockSpec((subs, 2 * n, 1), lambda i: (i, 0, 0)),
            whole(bank_hi),
            whole(bank_lo),
        ]
        + [whole(t) for t in tables],
        out_specs=pl.BlockSpec((2 * STOLT, groups, n), lambda i: (0, 0, 0)),
        out_shape=jax.ShapeDtypeStruct((2 * STOLT, groups, n), f32),
        scratch_shapes=[
            pltpu.VMEM((groups, x.shape[0], n), f32),
            pltpu.VMEM((groups, 2 * STOLT, n), f32),
        ],
        name="middle",
    )(x, cos_p, sin_p, hot, kind, bank_hi, bank_lo, *tables)


def quarter_tables():
    q = P_SIZE // 4
    m = np.arange(q)
    fwd, inv = [], []
    for low in range(4):
        a = 2 * np.pi / P_SIZE * (((4 * m[:, None] + low) * m[None, :]) % P_SIZE)
        fwd.append(np.concatenate([np.cos(a), np.sin(a)], 0))
        inv.append(np.concatenate([np.cos(a.T), np.sin(a.T)], 0) / P_SIZE)
    return np_split(np.stack(fwd)), np_split(np.stack(inv))


def swap_blocks(arrays):
    count = len(arrays)
    lanes = arrays[0].shape[-1]
    size = lanes // count
    block = lax.broadcasted_iota(jnp.int32, arrays[0].shape, 1) // size
    outs = []
    for b in range(count):
        acc = None
        for a in range(count):
            shift = (a - b) % count * size
            moved = pltpu.roll(arrays[a], shift, 1) if shift else arrays[a]
            acc = moved if acc is None else jnp.where(block == a, moved, acc)
        outs.append(acc)
    return outs


def azimuth_kernel(x, table, out):
    srcs, bins, lanes = x.shape
    half = lanes // 2
    low = lax.broadcasted_iota(jnp.int32, (bins, lanes), 1) < half
    quarters = []
    for q in range(4):
        a, b = x[2 * q], x[2 * q + 1]
        re = jnp.where(low, a, pltpu.roll(b, half, 1))
        im = jnp.where(low, pltpu.roll(a, half, 1), b)
        quarters.append((re, im))
    (r0, i0), (r1, i1), (r2, i2), (r3, i3) = quarters
    sr, si, dr, di = r0 + r2, i0 + i2, r0 - r2, i0 - i2
    tr, ti, er, ei = r1 + r3, i1 + i3, r1 - r3, i1 - i3
    mixed = (
        (sr + tr, si + ti),
        (dr + ei, di - er),
        (sr - tr, si - ti),
        (dr - ei, di + er),
    )
    size = P_SIZE // 4
    low = lax.broadcasted_iota(jnp.int32, (size, lanes), 1) < half
    rows = []
    for k in range(4):
        u = jnp.concatenate(mixed[k], 0)
        g = dots((table[0, k], table[1, k]), split(u), ((1,), (1,)))
        turned = pltpu.roll(g[size:], half, 1)
        rows.append(g[:size] + jnp.where(low, turned, -turned))
    for q, z in enumerate(swap_blocks(rows)):
        out[:, q] = z.reshape(out.shape[0], out.shape[2], lanes)


def image_kernel(x, table, out):
    devs, _, per, kh, lanes = x.shape
    size = P_SIZE // 4
    columns = [[] for _ in range(4)]
    for c in range(2):
        for h in range(per // 4):
            tiles = [x[:, c, 4 * h + j].reshape(devs * kh, lanes) for j in range(4)]
            for k, z in enumerate(swap_blocks(tiles)):
                columns[k].append(z)
    width = lanes * (per // 4)
    v = []
    for k in range(4):
        g = dots((table[0, k], table[1, k]), split(jnp.concatenate(columns[k], 1)), ((1,), (0,)))
        cos_g, sin_g = g[:size], g[size:]
        v.append((cos_g[:, :width] - sin_g[:, width:], cos_g[:, width:] + sin_g[:, :width]))
    (r0, i0), (r1, i1), (r2, i2), (r3, i3) = v
    sr, si, dr, di = r0 + r2, i0 + i2, r0 - r2, i0 - i2
    tr, ti, er, ei = r1 + r3, i1 + i3, r1 - r3, i1 - i3
    mixed = (
        (sr + tr, si + ti),
        (dr - ei, di + er),
        (sr - tr, si - ti),
        (dr + ei, di - er),
    )
    for q in range(4):
        for c in range(2):
            out[c, q * size : (q + 1) * size, :] = mixed[q][c]


def reference_phase(row_ids, cols):
    centered = (row_ids + P_SIZE // 2) % P_SIZE - P_SIZE // 2
    along_k = 2.0 * jnp.pi / (P_SIZE * SPACING) * centered.astype(f32)
    kr = 4.0 * jnp.pi / 3e8 * (9.6e9 + (cols.astype(f32) - F_LEN // 2) * (1.5e8 / F_LEN))
    squared = along_k * along_k
    depth = NEAR + B // 2
    return (
        -depth
        * squared[:, None]
        / (jnp.sqrt(kr[None, :] * kr[None, :] - squared[:, None]) + kr[None, :])
    )


def on_device(positions, amplitude, range_cells, bounce, stolt_block, kernel_choice, kernel_bank):
    n_pulse = lax.axis_size("pulse")
    n_scat = lax.axis_size("scat")
    n_dev = n_pulse * n_scat
    pulse_here = lax.axis_index("pulse")
    scat_here = lax.axis_index("scat")
    pulses = P_SIZE // n_pulse
    rows = P_SIZE // n_dev
    width = F_LEN // n_dev
    groups = rows // GROUP
    n = GROUP * BLOCKS
    bins_scat = B // n_scat
    bins_here = bins_scat // n_pulse

    ids = jnp.arange(GROUP, dtype=jnp.int32)[None, :, None] * BLOCKS
    first = stolt_block.reshape(groups, GROUP, BLOCKS) + ids
    pick = jnp.stack([first, first + 1], 1).reshape(groups, 2 * n, 1)
    hot = (pick == jnp.arange(n, dtype=jnp.int32)[None, None, :]).astype(bf16)
    kind = jnp.stack([kernel_choice.reshape(groups, n)] * 2, 1).reshape(groups, 2 * n, 1)
    bank_hi = lax.reduce_precision(kernel_bank, 8, 7)
    bank_lo = (kernel_bank - bank_hi).astype(bf16)
    bank_hi = bank_hi.astype(bf16)
    row_ids = (pulse_here * n_scat + scat_here) * rows + jnp.arange(rows, dtype=jnp.int32)
    theta = reference_phase(row_ids, jnp.arange(F_LEN, dtype=jnp.int32))
    theta = theta.reshape(rows * BLOCKS, STOLT)
    cos_p, sin_p = jnp.cos(theta), jnp.sin(theta)

    target = range_cells + SHIFT * bounce
    partial = binning(positions, amplitude, target, bounce, pulse_here * pulses, pulses)
    partial = partial.reshape(n_scat, bins_scat, 2 * pulses)
    binned = lax.dynamic_index_in_dim(partial, scat_here, 0, keepdims=False)
    for shift in range(1, n_scat):
        other = lax.dynamic_index_in_dim(
            partial, (scat_here + shift) % n_scat, 0, keepdims=False
        )
        ring = [(i, (i + shift) % n_scat) for i in range(n_scat)]
        binned = binned + lax.ppermute(other, "scat", ring)

    turned = lax.all_to_all(
        binned.reshape(n_pulse, bins_here, 2 * pulses), "pulse", 0, 0, tiled=True
    )
    per = STOLT // n_dev
    packed = 2 * pulses == 128 and 2 * bins_here == 128 and per % 4 == 0 and groups % 8 == 0
    if packed:
        forward, backward = (jnp.asarray(t) for t in quarter_tables())
        spectrum = pl.pallas_call(
            azimuth_kernel,
            out_shape=jax.ShapeDtypeStruct((n_dev, 4, groups, n), f32),
            name="azimuth",
        )(turned, forward)
        x = lax.all_to_all(spectrum, ("pulse", "scat"), 0, 0, tiled=True)
        x = x.reshape(4 * n_dev, groups, n)
        local = bins_here // BIN_SIDE
        i, s, c, l = np.meshgrid(
            np.arange(n_pulse), np.arange(n_scat), np.arange(2), np.arange(local), indexing="ij"
        )
        order = (c * BIN_SIDE + s * (BIN_SIDE // n_scat) + i * local + l).reshape(-1)
    else:
        turned = turned.reshape(n_pulse, bins_here, 2, pulses).transpose(0, 3, 2, 1)
        turned = turned.reshape(P_SIZE, 2 * bins_here)
        k = np.arange(P_SIZE)
        angle = 2 * np.pi / P_SIZE * ((k[:, None] * k[None, :]) % P_SIZE)
        az = jnp.asarray(np.concatenate([np.cos(angle), np.sin(angle)], 0), f32)
        product = jnp.dot(az, turned, precision=HIGH, preferred_element_type=f32)
        pc, ps = product[:P_SIZE], product[P_SIZE:]
        spectrum = pc + jnp.concatenate([ps[:, bins_here:], -ps[:, :bins_here]], 1)
        az_rows = lax.all_to_all(
            spectrum.reshape(n_dev, rows, 2 * bins_here), ("pulse", "scat"), 0, 0, tiled=True
        )
        x = az_rows.reshape(n_pulse, n_scat, rows, 2, bins_here).transpose(3, 1, 0, 4, 2)
        x = x.reshape(2, BIN_SIDE, BIN_SIDE, rows).transpose(0, 1, 3, 2)
        x = x.reshape(2 * BIN_SIDE, groups, n)
        order = np.arange(2 * BIN_SIDE)

    tables = tuple(jnp.asarray(t) for t in mid_tables(n_dev, order))
    ranged = middle(x, cos_p, sin_p, hot, kind, bank_hi, bank_lo, tables)
    if packed:
        columns = lax.all_to_all(
            ranged.reshape(n_dev, 2, per, groups, n), ("pulse", "scat"), 0, 0, tiled=True
        )
        return pl.pallas_call(
            image_kernel,
            out_shape=jax.ShapeDtypeStruct((2, P_SIZE, width), f32),
            name="image",
        )(columns, backward)
    columns = lax.all_to_all(
        ranged.reshape(n_dev, 2 * per, rows * BLOCKS), ("pulse", "scat"), 0, 0, tiled=True
    )
    columns = columns.reshape(n_dev, 2, per, rows, BLOCKS).transpose(0, 3, 1, 2, 4)
    columns = columns.reshape(P_SIZE, 2 * width)
    final = jnp.dot(az, columns, precision=HIGH, preferred_element_type=f32)
    fc, fs = final[:P_SIZE], final[P_SIZE:]
    re = (fc[:, :width] - fs[:, width:]) / P_SIZE
    im = (fc[:, width:] + fs[:, :width]) / P_SIZE
    return jnp.stack([re, im])


def solution(mesh):
    placed = (
        P(("scene", "scat")),
        P(None, ("scene", "scat")),
        P(("scene", "scat")),
        P(("scene", "scat")),
        P(("pulse", "scat"), None),
        P(("pulse", "scat"), None),
        P(),
    )
    return jax.shard_map(
        on_device,
        mesh=mesh,
        in_specs=placed,
        out_specs=P(None, "scene", ("pulse", "scat")),
        check_vma=False,
    )
```

```python
import functools

import jax
import jax.numpy as jnp
import numpy as np
from jax import lax
from jax.experimental import pallas as pl
from jax.experimental.pallas import tpu as pltpu
from jax.sharding import PartitionSpec as P

P_SIZE = 512
F_LEN = 4096
B = 1024
SHIFT = 16
STOLT = 128
BLOCKS = 32
SPACING = 2.0
NEAR = 700000.0
BIN_SIDE = 32
GROUP = 4
HIGH = lax.Precision.HIGH
f32 = jnp.float32
bf16 = jnp.bfloat16


def trig_coefs():
    x = np.cos(np.pi * (np.arange(400) + 0.5) / 400) * 0.5
    u = x * x
    s = np.polynomial.chebyshev.Chebyshev.fit(u, np.sin(np.pi * x) / x, 5).convert(
        kind=np.polynomial.Polynomial
    )
    c = np.polynomial.chebyshev.Chebyshev.fit(u, np.cos(np.pi * x), 5).convert(
        kind=np.polynomial.Polynomial
    )
    return [float(v) for v in s.coef], [float(v) for v in c.coef]


def horner(u, coefs):
    acc = jnp.full_like(u, coefs[-1])
    for c in coefs[-2::-1]:
        acc = acc * u + c
    return acc


def split(x):
    hi = x.astype(bf16)
    lo = (x - hi.astype(f32)).astype(bf16)
    return hi, lo


def np_split(x):
    x = np.asarray(x, np.float64)
    hi = np.asarray(x, jnp.bfloat16)
    lo = np.asarray(x - hi.astype(np.float64), jnp.bfloat16)
    return np.stack([hi, lo])


def dots(a, b, dims):
    d = functools.partial(
        lax.dot_general, dimension_numbers=(dims, ((), ())), preferred_element_type=f32
    )
    return d(a[0], b[0]) + (d(a[0], b[1]) + d(a[1], b[0]))


def bin_kernel(pulse_base, pos, amp, tgt, bnc, out, acc, *, pulses, sin_c, cos_c):
    step = pl.program_id(0)
    width = pos.shape[1]

    @pl.when(step == 0)
    def _():
        acc[...] = jnp.zeros_like(acc)

    base = pulse_base[0]
    ids = base + lax.broadcasted_iota(jnp.int32, (pulses, width), 0)
    along = (ids.astype(f32) - P_SIZE // 2) * SPACING
    target = tgt[...] + SHIFT * bnc[...]
    slant = NEAR + target.astype(f32)
    offset = along - pos[...]
    square = offset * offset
    excess = square / (jnp.sqrt(slant * slant + square) + slant)
    halves = excess * -128.0
    whole = jnp.round(halves)
    r = halves - whole
    u = r * r
    odd = whole - 2.0 * jnp.floor(whole * 0.5)
    sign = 1.0 - 2.0 * odd
    sin_p = sign * r * horner(u, sin_c)
    cos_p = sign * horner(u, cos_c)
    flip = 1.0 - 2.0 * bnc[...].astype(f32)
    are = flip * amp[0:1]
    aim = flip * amp[1:2]
    re = are * cos_p - aim * sin_p
    im = are * sin_p + aim * cos_p
    steer = jnp.concatenate([re, im], 0)
    hi, lo = split(steer)
    rhs = jnp.concatenate([hi, lo], 0)
    bins = lax.broadcasted_iota(jnp.int32, (B, width), 0)
    hot = jnp.where(bins == target, 1.0, 0.0).astype(bf16)
    acc[...] += lax.dot_general(
        hot, rhs, (((1,), (1,)), ((), ())), preferred_element_type=f32
    )

    @pl.when(step == pl.num_programs(0) - 1)
    def _():
        out[...] = acc[:, : 2 * pulses] + acc[:, 2 * pulses :]


def binning(positions, amplitude, cells, bounce, pulse_base, pulses):
    count = positions.shape[0]
    width = min(2048, count)
    sin_c, cos_c = trig_coefs()
    row = lambda n: pl.BlockSpec((n, width), lambda i: (0, i))
    return pl.pallas_call(
        functools.partial(bin_kernel, pulses=pulses, sin_c=sin_c, cos_c=cos_c),
        grid=(count // width,),
        in_specs=[pl.BlockSpec(memory_space=pltpu.SMEM), row(1), row(2), row(1), row(1)],
        out_specs=pl.BlockSpec((B, 2 * pulses), lambda i: (0, 0)),
        out_shape=jax.ShapeDtypeStruct((B, 2 * pulses), f32),
        scratch_shapes=[pltpu.VMEM((B, 4 * pulses), f32)],
        name="binning",
    )(
        pulse_base.reshape(1),
        positions.reshape(1, count),
        amplitude,
        cells.reshape(1, count),
        bounce.reshape(1, count),
    )


def complex_rows(c, s):
    return np.block([[c, s], [-s, c]])


def mid_tables(n_dev, order):
    side = np.arange(BIN_SIDE)
    t = np.arange(STOLT)
    eye = np.eye(GROUP)
    a = -2 * np.pi / STOLT * ((side[:, None] * t[None, :]) % STOLT)
    ta = complex_rows(np.cos(a), np.sin(a))[order]
    a = -2 * np.pi / F_LEN * (side[:, None] * t[None, :])
    wa = np.stack([np.tile(np.cos(a), (GROUP, 1)), np.tile(np.sin(a), (GROUP, 1))])
    a = -2 * np.pi / BIN_SIDE * ((side[:, None] * side[None, :]) % BIN_SIDE)
    c, s = np.kron(eye, np.cos(a)), np.kron(eye, np.sin(a))
    tb = complex_rows(c, s).T
    blk = np.arange(BLOCKS)
    a = 2 * np.pi / BLOCKS * ((blk[:, None] * blk[None, :]) % BLOCKS)
    c, s = np.kron(eye, np.cos(a)), np.kron(eye, np.sin(a))
    tc = complex_rows(c, s)
    a = 2 * np.pi / F_LEN * (t[:, None] * blk[None, :])
    wc = np.stack([np.tile(np.cos(a), (1, GROUP)), np.tile(np.sin(a), (1, GROUP))])
    a = 2 * np.pi / STOLT * ((t[:, None] * t[None, :]) % STOLT)
    td = complex_rows(np.cos(a), np.sin(a)).T / F_LEN
    td = td.reshape(2, n_dev, STOLT // n_dev, 2 * STOLT).transpose(1, 0, 2, 3)
    td = td.reshape(2 * STOLT, 2 * STOLT)
    return (
        np_split(ta),
        wa.astype(np.float32),
        np_split(tb),
        np_split(tc),
        wc.astype(np.float32),
        np_split(td),
    )


def mid_kernel(
    x, cos_p, sin_p, hot, kind, bank_hi, bank_lo, ta, wa, tb, tc, wc, td, out, xs, os, *, subs
):
    n = GROUP * BLOCKS
    step = pl.program_id(0)
    groups = x.shape[1]

    @pl.when(step == 0)
    def _():
        for g in range(groups):
            xs[g] = x[:, g, :]

    parts_hi, parts_lo = [], []
    for g in range(subs):
        lanes = slice(g * n, (g + 1) * n)
        y = dots(split(xs[step * subs + g]), (ta[0], ta[1]), ((0,), (0,)))
        yr, yi = y[:, :STOLT], y[:, STOLT:]
        y = jnp.concatenate([yr * wa[0] - yi * wa[1], yr * wa[1] + yi * wa[0]], 0)
        z = dots((tb[0], tb[1]), split(y), ((1,), (0,)))
        zr, zi = z[:n], z[n:]
        cp, sp = cos_p[lanes], sin_p[lanes]
        z = jnp.concatenate([zr * cp - zi * sp, zr * sp + zi * cp], 1)
        hi, lo = split(z)
        picked = jnp.dot(
            hot[g], jnp.concatenate([hi, lo], 1), preferred_element_type=f32
        ).astype(bf16)
        first, second = picked[:n], picked[n:]
        for c in range(2):
            for base, keep in ((0, parts_hi), (2 * STOLT, parts_lo)):
                cut = slice(base + c * STOLT, base + (c + 1) * STOLT)
                keep.append(jnp.concatenate([first[:, cut], second[:, cut]], 1))
    ghi = jnp.concatenate(parts_hi, 0)
    glo = jnp.concatenate(parts_lo, 0)
    kinds = kind[...].reshape(subs * 2 * n, 1)
    kinds = jnp.broadcast_to(kinds, (subs * 2 * n, STOLT))
    acc = jnp.zeros((subs * 2 * n, STOLT), f32)
    for k in range(0, bank_hi.shape[0], 2):
        khi = jnp.concatenate([bank_hi[k], bank_hi[k + 1]], 1)
        klo = jnp.concatenate([bank_lo[k], bank_lo[k + 1]], 1)
        r = dots((ghi, glo), (khi, klo), ((1,), (0,)))
        for half in range(2):
            acc = jnp.where(kinds == k + half, r[:, half * STOLT : (half + 1) * STOLT], acc)
    for g in range(subs):
        s = acc[g * 2 * n : (g + 1) * 2 * n]
        y = dots(split(s), (tc[0], tc[1]), ((0,), (0,)))
        yr, yi = y[:, :n], y[:, n:]
        y = jnp.concatenate([yr * wc[0] - yi * wc[1], yr * wc[1] + yi * wc[0]], 0)
        os[step * subs + g] = dots((td[0], td[1]), split(y), ((1,), (0,)))

    @pl.when(step == pl.num_programs(0) - 1)
    def _():
        for g in range(groups):
            out[:, g, :] = os[g]


def middle(x, cos_p, sin_p, hot, kind, bank_hi, bank_lo, tables):
    groups = x.shape[1]
    subs = min(4, groups)
    n = GROUP * BLOCKS
    whole = lambda a: pl.BlockSpec(a.shape, lambda i: (0,) * a.ndim)
    return pl.pallas_call(
        functools.partial(mid_kernel, subs=subs),
        grid=(groups // subs,),
        in_specs=[
            whole(x),
            pl.BlockSpec((subs * n, STOLT), lambda i: (i, 0)),
            pl.BlockSpec((subs * n, STOLT), lambda i: (i, 0)),
            pl.BlockSpec((subs, 2 * n, n), lambda i: (i, 0, 0)),
            pl.BlockSpec((subs, 2 * n, 1), lambda i: (i, 0, 0)),
            whole(bank_hi),
            whole(bank_lo),
        ]
        + [whole(t) for t in tables],
        out_specs=pl.BlockSpec((2 * STOLT, groups, n), lambda i: (0, 0, 0)),
        out_shape=jax.ShapeDtypeStruct((2 * STOLT, groups, n), f32),
        scratch_shapes=[
            pltpu.VMEM((groups, x.shape[0], n), f32),
            pltpu.VMEM((groups, 2 * STOLT, n), f32),
        ],
        name="middle",
    )(x, cos_p, sin_p, hot, kind, bank_hi, bank_lo, *tables)


def quarter_tables():
    q = P_SIZE // 4
    m = np.arange(q)
    fwd, inv = [], []
    for low in range(4):
        a = 2 * np.pi / P_SIZE * (((4 * m[:, None] + low) * m[None, :]) % P_SIZE)
        fwd.append(np.concatenate([np.cos(a), np.sin(a)], 0))
        inv.append(np.concatenate([np.cos(a.T), np.sin(a.T)], 0) / P_SIZE)
    return np_split(np.stack(fwd)), np_split(np.stack(inv))


def swap_blocks(arrays):
    count = len(arrays)
    lanes = arrays[0].shape[-1]
    size = lanes // count
    block = lax.broadcasted_iota(jnp.int32, arrays[0].shape, 1) // size
    outs = []
    for b in range(count):
        acc = None
        for a in range(count):
            shift = (a - b) % count * size
            moved = pltpu.roll(arrays[a], shift, 1) if shift else arrays[a]
            acc = moved if acc is None else jnp.where(block == a, moved, acc)
        outs.append(acc)
    return outs


def azimuth_kernel(x, table, out):
    srcs, bins, lanes = x.shape
    half = lanes // 2
    low = lax.broadcasted_iota(jnp.int32, (bins, lanes), 1) < half
    quarters = []
    for q in range(4):
        a, b = x[2 * q], x[2 * q + 1]
        re = jnp.where(low, a, pltpu.roll(b, half, 1))
        im = jnp.where(low, pltpu.roll(a, half, 1), b)
        quarters.append((re, im))
    (r0, i0), (r1, i1), (r2, i2), (r3, i3) = quarters
    sr, si, dr, di = r0 + r2, i0 + i2, r0 - r2, i0 - i2
    tr, ti, er, ei = r1 + r3, i1 + i3, r1 - r3, i1 - i3
    mixed = (
        (sr + tr, si + ti),
        (dr + ei, di - er),
        (sr - tr, si - ti),
        (dr - ei, di + er),
    )
    size = P_SIZE // 4
    low = lax.broadcasted_iota(jnp.int32, (size, lanes), 1) < half
    rows = []
    for k in range(4):
        u = jnp.concatenate(mixed[k], 0)
        g = dots((table[0, k], table[1, k]), split(u), ((1,), (1,)))
        turned = pltpu.roll(g[size:], half, 1)
        rows.append(g[:size] + jnp.where(low, turned, -turned))
    for q, z in enumerate(swap_blocks(rows)):
        out[:, q] = z.reshape(out.shape[0], out.shape[2], lanes)


def image_kernel(x, table, out):
    devs, _, per, kh, lanes = x.shape
    size = P_SIZE // 4
    columns = [[] for _ in range(4)]
    for c in range(2):
        for h in range(per // 4):
            tiles = [x[:, c, 4 * h + j].reshape(devs * kh, lanes) for j in range(4)]
            for k, z in enumerate(swap_blocks(tiles)):
                columns[k].append(z)
    width = lanes * (per // 4)
    v = []
    for k in range(4):
        g = dots((table[0, k], table[1, k]), split(jnp.concatenate(columns[k], 1)), ((1,), (0,)))
        cos_g, sin_g = g[:size], g[size:]
        v.append((cos_g[:, :width] - sin_g[:, width:], cos_g[:, width:] + sin_g[:, :width]))
    (r0, i0), (r1, i1), (r2, i2), (r3, i3) = v
    sr, si, dr, di = r0 + r2, i0 + i2, r0 - r2, i0 - i2
    tr, ti, er, ei = r1 + r3, i1 + i3, r1 - r3, i1 - i3
    mixed = (
        (sr + tr, si + ti),
        (dr - ei, di + er),
        (sr - tr, si - ti),
        (dr + ei, di - er),
    )
    for q in range(4):
        for c in range(2):
            out[c, q * size : (q + 1) * size, :] = mixed[q][c]


def reference_phase(row_ids, cols):
    centered = (row_ids + P_SIZE // 2) % P_SIZE - P_SIZE // 2
    along_k = 2.0 * jnp.pi / (P_SIZE * SPACING) * centered.astype(f32)
    kr = 4.0 * jnp.pi / 3e8 * (9.6e9 + (cols.astype(f32) - F_LEN // 2) * (1.5e8 / F_LEN))
    squared = along_k * along_k
    depth = NEAR + B // 2
    return (
        -depth
        * squared[:, None]
        / (jnp.sqrt(kr[None, :] * kr[None, :] - squared[:, None]) + kr[None, :])
    )


def on_device(positions, amplitude, range_cells, bounce, stolt_block, kernel_choice, kernel_bank):
    n_pulse = lax.axis_size("pulse")
    n_scat = lax.axis_size("scat")
    n_dev = n_pulse * n_scat
    pulse_here = lax.axis_index("pulse")
    scat_here = lax.axis_index("scat")
    pulses = P_SIZE // n_pulse
    rows = P_SIZE // n_dev
    width = F_LEN // n_dev
    groups = rows // GROUP
    n = GROUP * BLOCKS
    bins_scat = B // n_scat
    bins_here = bins_scat // n_pulse

    ids = jnp.arange(GROUP, dtype=jnp.int32)[None, :, None] * BLOCKS
    first = stolt_block.reshape(groups, GROUP, BLOCKS) + ids
    pick = jnp.stack([first, first + 1], 1).reshape(groups, 2 * n, 1)
    hot = (pick == jnp.arange(n, dtype=jnp.int32)[None, None, :]).astype(bf16)
    kind = jnp.stack([kernel_choice.reshape(groups, n)] * 2, 1).reshape(groups, 2 * n, 1)
    bank_hi = lax.reduce_precision(kernel_bank, 8, 7)
    bank_lo = (kernel_bank - bank_hi).astype(bf16)
    bank_hi = bank_hi.astype(bf16)
    row_ids = (pulse_here * n_scat + scat_here) * rows + jnp.arange(rows, dtype=jnp.int32)
    theta = reference_phase(row_ids, jnp.arange(F_LEN, dtype=jnp.int32))
    theta = theta.reshape(rows * BLOCKS, STOLT)
    cos_p, sin_p = jnp.cos(theta), jnp.sin(theta)

    partial = binning(positions, amplitude, range_cells, bounce, pulse_here * pulses, pulses)
    partial = partial.reshape(n_scat, bins_scat, 2 * pulses)
    binned = lax.dynamic_index_in_dim(partial, scat_here, 0, keepdims=False)
    for shift in range(1, n_scat):
        other = lax.dynamic_index_in_dim(
            partial, (scat_here + shift) % n_scat, 0, keepdims=False
        )
        ring = [(i, (i + shift) % n_scat) for i in range(n_scat)]
        binned = binned + lax.ppermute(other, "scat", ring)

    turned = lax.all_to_all(
        binned.reshape(n_pulse, bins_here, 2 * pulses), "pulse", 0, 0, tiled=True
    )
    per = STOLT // n_dev
    packed = 2 * pulses == 128 and 2 * bins_here == 128 and per % 4 == 0 and groups % 8 == 0
    if packed:
        forward, backward = (jnp.asarray(t) for t in quarter_tables())
        spectrum = pl.pallas_call(
            azimuth_kernel,
            out_shape=jax.ShapeDtypeStruct((n_dev, 4, groups, n), f32),
            name="azimuth",
        )(turned, forward)
        x = lax.all_to_all(spectrum, ("pulse", "scat"), 0, 0, tiled=True)
        x = x.reshape(4 * n_dev, groups, n)
        local = bins_here // BIN_SIDE
        i, s, c, l = np.meshgrid(
            np.arange(n_pulse), np.arange(n_scat), np.arange(2), np.arange(local), indexing="ij"
        )
        order = (c * BIN_SIDE + s * (BIN_SIDE // n_scat) + i * local + l).reshape(-1)
    else:
        turned = turned.reshape(n_pulse, bins_here, 2, pulses).transpose(0, 3, 2, 1)
        turned = turned.reshape(P_SIZE, 2 * bins_here)
        k = np.arange(P_SIZE)
        angle = 2 * np.pi / P_SIZE * ((k[:, None] * k[None, :]) % P_SIZE)
        az = jnp.asarray(np.concatenate([np.cos(angle), np.sin(angle)], 0), f32)
        product = jnp.dot(az, turned, precision=HIGH, preferred_element_type=f32)
        pc, ps = product[:P_SIZE], product[P_SIZE:]
        spectrum = pc + jnp.concatenate([ps[:, bins_here:], -ps[:, :bins_here]], 1)
        az_rows = lax.all_to_all(
            spectrum.reshape(n_dev, rows, 2 * bins_here), ("pulse", "scat"), 0, 0, tiled=True
        )
        x = az_rows.reshape(n_pulse, n_scat, rows, 2, bins_here).transpose(3, 1, 0, 4, 2)
        x = x.reshape(2, BIN_SIDE, BIN_SIDE, rows).transpose(0, 1, 3, 2)
        x = x.reshape(2 * BIN_SIDE, groups, n)
        order = np.arange(2 * BIN_SIDE)

    tables = tuple(jnp.asarray(t) for t in mid_tables(n_dev, order))
    ranged = middle(x, cos_p, sin_p, hot, kind, bank_hi, bank_lo, tables)
    if packed:
        columns = lax.all_to_all(
            ranged.reshape(n_dev, 2, per, groups, n), ("pulse", "scat"), 0, 0, tiled=True
        )
        return pl.pallas_call(
            image_kernel,
            out_shape=jax.ShapeDtypeStruct((2, P_SIZE, width), f32),
            name="image",
        )(columns, backward)
    columns = lax.all_to_all(
        ranged.reshape(n_dev, 2 * per, rows * BLOCKS), ("pulse", "scat"), 0, 0, tiled=True
    )
    columns = columns.reshape(n_dev, 2, per, rows, BLOCKS).transpose(0, 3, 1, 2, 4)
    columns = columns.reshape(P_SIZE, 2 * width)
    final = jnp.dot(az, columns, precision=HIGH, preferred_element_type=f32)
    fc, fs = final[:P_SIZE], final[P_SIZE:]
    re = (fc[:, :width] - fs[:, width:]) / P_SIZE
    im = (fc[:, width:] + fs[:, :width]) / P_SIZE
    return jnp.stack([re, im])


def solution(mesh):
    placed = (
        P(("scene", "scat")),
        P(None, ("scene", "scat")),
        P(("scene", "scat")),
        P(("scene", "scat")),
        P(("pulse", "scat"), None),
        P(("pulse", "scat"), None),
        P(),
    )
    return jax.shard_map(
        on_device,
        mesh=mesh,
        in_specs=placed,
        out_specs=P(None, "scene", ("pulse", "scat")),
        check_vma=False,
    )
```
